32 devices in a mesh: grp: 4 (over z), inner: 8 (over y, x, core).
Axes of the slice: x: 2, y: 2, z: 4, core: 2. Of those that a mesh axis runs over, the one named last changes fastest.
Arguments:
- queries: bfloat16 [256, 64, 192], P('inner', 'grp'), may hold values from -300 to 300
- tenant_ids: int32 [256], replicated, may hold values from 0 to 3
- prefix_lengths: int32 [4], replicated, may hold values from 2 to 1024, as said below
- latent_cache: bfloat16 [1024, 576], P('inner'), may hold values from -8 to 8
- key_absorb: bfloat16 [64, 128, 512], P('grp'), may hold values from -0.5 to 0.5
- value_absorb: bfloat16 [64, 512, 128], P('grp'), may hold values from -12 to 12
- key_down: bfloat16 [4, 64, 128, 16], P(None, 'grp'), may hold values from -0.5 to 0.5
- key_up: bfloat16 [4, 64, 16, 512], P(None, 'grp'), may hold values from -1.5 to 1.5
- value_down: bfloat16 [4, 64, 512, 16], P(None, 'grp'), may hold values from -6 to 6
- value_up: bfloat16 [4, 64, 16, 128], P(None, 'grp'), may hold values from -1.5 to 1.5
- out_proj: bfloat16 [8192, 7168], P('grp', 'inner'), may hold values from -0.0625 to 0.0625
Outputs:
- attended: bfloat16 [256, 7168], P('grp', 'inner')
The draws below stay inside these ranges and needn't reach their ends.
Inputs may be any that keep to these rules, and one draw needn't show every extreme that they name: `prefix_lengths`: at least one tenant sees all 1024 positions.
All inputs are finite; a program needn't handle non-finite values.
Results may differ from the reference program's by a relative error of at most 0.011.
Values may be sent and summed in bfloat16 or wider, within the bound.
No kernel may reach another device: no remote copies, remote signals or barrier semaphores. Data moves between devices by JAX's collectives and lax.ppermute only.
A program may use at most 64 MiB of HBM per device.

```python
import jax
import jax.numpy as jnp
from jax import lax

D = 7168
HEADS = 64
LAT = 512
ROPE = 64
NOPE = 128
VDIM = 128
RANK = 16
TENANTS = 4
TQ = 256
CTX_DEV = 128
CTX = 1024
N_INNER = 8


def draw_latent_cache(key, part):
    inner_key = jax.random.fold_in(key, 23)
    values = jnp.clip(jax.random.normal(jax.random.fold_in(inner_key, 3), (CTX, LAT + ROPE), jnp.float32), -6.0, 6.0)
    return values.astype(jnp.bfloat16)


def draw_queries(key, part):
    inner_key = jax.random.fold_in(key, 41)
    values = jnp.clip(jax.random.normal(jax.random.fold_in(inner_key, 3), (TQ, HEADS, NOPE + ROPE), jnp.float32), -6.0, 6.0)
    return values.astype(jnp.bfloat16)


def draw_prefix_lengths(key, part):
    lengths = jax.random.randint(jax.random.fold_in(key, 31), (TENANTS,), 2, CTX + 1, jnp.int32)
    widest = jax.random.randint(jax.random.fold_in(key, 32), (), 0, TENANTS, jnp.int32)
    return jnp.where(jnp.arange(TENANTS, dtype=jnp.int32) == widest, CTX, lengths).astype(jnp.int32)


def plant(entries, key, low, largest):
    longest = entries.shape.index(max(entries.shape))
    spots = []
    for shift in (0, 1):
        where = [jax.random.randint(jax.random.fold_in(key, axis), (), 0, length) for axis, length in enumerate(entries.shape)]
        where[longest] = (where[longest] + shift) % entries.shape[longest]
        spots.append(tuple(where))
    return entries.at[spots[0]].set(low).at[spots[1]].set(largest)


def block_levels(key, dims, pieces, low, high):
    level, own = 1.0, jax.random.fold_in(key, 6)
    for axis_at, parts in pieces:
        heights = jnp.exp(jax.random.uniform(jax.random.fold_in(own, axis_at), (parts,), jnp.float32, low / len(pieces), high / len(pieces)))
        level = level * jnp.repeat(heights, dims[axis_at] // parts).reshape([-1 if axis == axis_at else 1 for axis in range(len(dims))])
    return level


def centred(key, shape, spread, limit, cuts=(), kind=jnp.bfloat16):
    loudness = block_levels(key, shape, cuts, -0.22, 0.18) if cuts else 1.0
    array = jax.random.normal(key, shape, jnp.float32) * spread * loudness
    return jnp.minimum(jnp.maximum(array, -limit), limit).astype(kind)


def setup_inputs(seed: int = 0) -> dict:
    seeds = jax.random.split(jax.random.key(seed), 12)
    queries = draw_queries(jax.random.fold_in(seeds[11], 71), 0)
    tenant_ids = plant(jax.random.randint(seeds[1], (TQ,), 0, TENANTS), jax.random.fold_in(seeds[1], 1), 0, TENANTS - 1).astype(jnp.int32)
    prefix_lengths = draw_prefix_lengths(jax.random.fold_in(seeds[11], 71), 0)
    latent_cache = draw_latent_cache(jax.random.fold_in(seeds[11], 71), 0)
    key_absorb = centred(seeds[4], (HEADS, NOPE, LAT), NOPE ** -0.5, 0.5, ((0, 4),))
    value_absorb = centred(seeds[5], (HEADS, LAT, VDIM), 2.0, 12.0, ((0, 4),))
    key_down = centred(seeds[6], (TENANTS, HEADS, NOPE, RANK), NOPE ** -0.5, 0.5, ((1, 4),))
    key_up = centred(seeds[7], (TENANTS, HEADS, RANK, LAT), RANK ** -0.5, 1.5, ((1, 4),))
    value_down = centred(seeds[8], (TENANTS, HEADS, LAT, RANK), 1.0, 6.0, ((1, 4),))
    value_up = centred(seeds[9], (TENANTS, HEADS, RANK, VDIM), RANK ** -0.5, 1.5, ((1, 4),))
    out_proj = centred(seeds[10], (HEADS * VDIM, D), (HEADS * VDIM) ** -0.5, 0.0625, ((0, 4), (1, 8)))
    return dict(queries=queries, tenant_ids=tenant_ids, prefix_lengths=prefix_lengths, latent_cache=latent_cache, key_absorb=key_absorb, value_absorb=value_absorb, key_down=key_down, key_up=key_up, value_down=value_down, value_up=value_up, out_proj=out_proj)


masked_score = -30000.0


def absorb(queries, chosen, key_absorb, key_down, key_up):
    nope_part = queries[:, :, :NOPE].astype(jnp.float32)
    rope_part = queries[:, :, NOPE:].astype(jnp.float32)
    latent = jnp.einsum("thn,hnc->thc", nope_part, key_absorb.astype(jnp.float32))
    lowrank = jnp.einsum("thn,khnr->thkr", nope_part, key_down.astype(jnp.float32)) * chosen[:, None, :, None]
    lowrank = lowrank.astype(jnp.bfloat16).astype(jnp.float32)
    latent = latent + jnp.einsum("thkr,khrc->thc", lowrank, key_up.astype(jnp.float32))
    return jnp.concatenate([latent, rope_part], axis=2).astype(jnp.bfloat16)


def reference(queries, tenant_ids, prefix_lengths, latent_cache, key_absorb, value_absorb, key_down, key_up, value_down, value_up, out_proj):
    table = tenant_ids[:, None] == jnp.arange(TENANTS, dtype=jnp.int32)[None, :]
    chosen = table.astype(jnp.float32)
    limits = jnp.sum(jnp.where(table, prefix_lengths[None, :], 0), axis=1).astype(jnp.int32)
    query_full = absorb(queries, chosen, key_absorb, key_down, key_up).astype(jnp.float32)
    scale = (NOPE + ROPE) ** -0.5

    def one_block(block):
        start = (block * CTX_DEV).astype(jnp.int32)
        cache_block = lax.dynamic_slice_in_dim(latent_cache, start, CTX_DEV, 0).astype(jnp.float32)
        scores = jnp.einsum("thc,jc->thj", query_full, cache_block) * scale
        positions = start + jnp.arange(CTX_DEV, dtype=jnp.int32)
        allowed = (positions[None, :] < limits[:, None])[:, None, :]
        masked = jnp.where(allowed, scores, masked_score)
        block_max = jnp.max(masked, axis=2)
        weights = jnp.where(allowed, jnp.exp(masked - block_max[:, :, None]), 0.0)
        block_sum = jnp.sum(weights, axis=2)
        rounded = weights.astype(jnp.bfloat16).astype(jnp.float32)
        block_latent = jnp.einsum("thj,jc->thc", rounded, cache_block[:, :LAT]).astype(jnp.bfloat16).astype(jnp.float32)
        values = jnp.einsum("thc,hcv->thv", block_latent, value_absorb.astype(jnp.float32))
        lowrank = jnp.einsum("thc,khcr->thkr", block_latent, value_down.astype(jnp.float32)) * chosen[:, None, :, None]
        lowrank = lowrank.astype(jnp.bfloat16).astype(jnp.float32)
        values = values + jnp.einsum("thkr,khrv->thv", lowrank, value_up.astype(jnp.float32))
        return block_max, block_sum, values

    block_max, block_sum, values = lax.map(one_block, jnp.arange(N_INNER, dtype=jnp.int32))
    peak = jnp.max(block_max, axis=0)
    factor = jnp.exp(block_max - peak[None])
    numer = jnp.sum(values * factor[..., None], axis=0)
    denom = jnp.sum(block_sum * factor, axis=0)
    head_out = (numer / denom[:, :, None]).astype(jnp.bfloat16)
    flat = head_out.reshape(TQ, HEADS * VDIM)
    return jnp.dot(flat, out_proj, preferred_element_type=jnp.float32).astype(jnp.bfloat16)
```

```python
import functools

import jax
import jax.numpy as jnp
from jax import lax
from jax.experimental import pallas as pl
from jax.experimental.pallas import tpu as pltpu
from jax.sharding import PartitionSpec as P

LAT = 512
ROPE = 64
NOPE = 128


BF16 = jnp.bfloat16
F32 = jnp.float32
LOG2E = 1.4426950408889634
HIDDEN = -1e30

VMEM = pltpu.MemorySpace.VMEM
SMEM = pltpu.MemorySpace.SMEM
HBM = pltpu.MemorySpace.HBM


def dot(a, b):
    return jnp.dot(a, b, preferred_element_type=F32)


def dot_nt(a, b):
    return lax.dot_general(a, b, (((1,), (1,)), ((), ())), preferred_element_type=F32)


def absorb_kernel(core_ref, own_ref, pair_ref, chosen_ref, absorb_ref, down_ref, up_ref, out_ref, plain, turned):
    own_rows, heads, _ = own_ref.shape
    half, _, lat = absorb_ref.shape
    tenants, _, rank, nope = down_ref.shape
    rows = 2 * own_rows
    core = core_ref[0]
    span = own_rows * heads
    for ref, side in ((own_ref, core), (pair_ref, 1 - core)):
        first = pl.multiple_of(side * span, 8)
        if heads % 16 == 0:
            whole = ref[...].reshape(span, ref.shape[2]).astype(F32)
            plain[pl.ds(first, span), :] = whole[:, :nope]
            turned[pl.ds(first, span), : whole.shape[1] - nope] = whole[:, nope:]
        else:
            for row in range(own_rows):
                one = ref[row].astype(F32)
                plain[pl.ds(side * span + row * heads, heads), :] = one[:, :nope]
                turned[pl.ds(side * span + row * heads, heads), : one.shape[1] - nope] = one[:, nope:]
    chosen = chosen_ref[...]
    for head in range(half):
        picked = pl.ds(core * half + head, rows, stride=heads)
        nope_part = plain[picked, :].astype(BF16)
        down = down_ref[:, head].reshape(tenants * rank, nope)
        up = up_ref[:, head].reshape(tenants * rank, lat)
        low = (dot_nt(nope_part, down) * chosen).astype(BF16)
        latent = dot(nope_part, absorb_ref[head]) + dot(low, up)
        out_ref[head * rows : (head + 1) * rows, :lat] = latent.astype(BF16)
        out_ref[head * rows : (head + 1) * rows, lat:] = turned[picked, :][:, : out_ref.shape[1] - lat].astype(BF16)


def attend_kernel(blocks, scale, place_ref, query_ref, limit_ref, chosen_ref, *refs):
    cache = refs[:blocks]
    absorb_hbm, down_hbm, up_hbm, out_ref, score, weight, absorb_ref, down_ref, up_ref, sems = refs[blocks:]
    half = absorb_ref.shape[0]
    lat = absorb_ref.shape[1]
    vdim = absorb_ref.shape[2]
    tenants, _, rank, _ = down_ref.shape
    rows = limit_ref.shape[0]
    span = cache[0].shape[1]
    first = place_ref[blocks] * half
    copies = [
        pltpu.make_async_copy(absorb_hbm.at[pl.ds(first, half)], absorb_ref, sems.at[0]),
        pltpu.make_async_copy(down_hbm.at[:, pl.ds(first, half)], down_ref, sems.at[1]),
        pltpu.make_async_copy(up_hbm.at[:, pl.ds(first, half)], up_ref, sems.at[2]),
    ]
    for copy in copies:
        copy.start()

    keys = jnp.concatenate([ref[...] for ref in cache], axis=1)
    score[...] = dot(query_ref[...], keys)

    step = min(rows, 32)
    total = []
    for start in range(0, half * rows, step):
        token = start % rows
        limit = limit_ref[token : token + step, :]
        lane = lax.broadcasted_iota(jnp.int32, (step, span), 1)
        allowed = [lane + place_ref[block] * span < limit for block in range(blocks)]
        scores = [
            jnp.where(allowed[block], score[start : start + step, block * span : (block + 1) * span], HIDDEN)
            for block in range(blocks)
        ]
        peak = scores[0]
        for block in range(1, blocks):
            peak = jnp.maximum(peak, scores[block])
        peak = jnp.max(peak, axis=1, keepdims=True)
        mass = jnp.zeros((step, span), F32)
        for block in range(blocks):
            part = jnp.where(allowed[block], jnp.exp2((scores[block] - peak) * (scale * LOG2E)), 0.0)
            mass = mass + part
            weight[start : start + step, block * span : (block + 1) * span] = part.astype(BF16)
        total.append(jnp.sum(mass, axis=1, keepdims=True))
    total = jnp.concatenate(total, axis=0)

    latents = jnp.concatenate([ref[:lat, :] for ref in cache], axis=1)
    mixed = (dot_nt(weight[...], latents) / total).astype(BF16)

    for copy in copies:
        copy.wait()
    chosen = chosen_ref[...]
    for head in range(half):
        latent = mixed[head * rows : (head + 1) * rows, :]
        down = down_ref[:, head].reshape(tenants * rank, lat)
        up = up_ref[:, head].reshape(tenants * rank, vdim)
        low = (dot_nt(latent, down) * chosen).astype(BF16)
        value = dot(latent, absorb_ref[head]) + dot(low, up)
        out_ref[:, head * vdim : (head + 1) * vdim] = value.astype(BF16)


def project_kernel(pairs, groups, place_ref, *refs):
    same = refs[:pairs]
    other = refs[pairs : 2 * pairs]
    weight_ref, keep_ref, send_ref, flat = refs[2 * pairs :]
    rows, width = same[0].shape
    core, pair, group = place_ref[0], place_ref[1], place_ref[2]
    for distance in range(pairs):
        row = pl.multiple_of((pair ^ distance) * rows, rows)
        flat[pl.ds(row, rows), pl.ds(pl.multiple_of(core * width, width), width)] = same[distance][...]
        flat[pl.ds(row, rows), pl.ds(pl.multiple_of((1 - core) * width, width), width)] = other[distance][...]
    chunk = flat.shape[0] // groups
    left = jnp.concatenate(
        [
            flat[pl.ds(pl.multiple_of((group ^ distance) * chunk, chunk), chunk), :]
            for distance in range(groups)
        ],
        axis=0,
    )
    product = dot(left, weight_ref[...])
    keep_ref[...] = product[:chunk]
    for distance in range(1, groups):
        send_ref[distance - 1] = product[distance * chunk : (distance + 1) * chunk].astype(BF16)


def spec(space):
    return pl.BlockSpec(memory_space=space)


def cost(flops, moved):
    return pl.CostEstimate(flops=int(flops), bytes_accessed=int(moved), transcendentals=0)


def local(
    n_inner,
    n_grp,
    queries,
    tenant_ids,
    prefix_lengths,
    latent_cache,
    key_absorb,
    value_absorb,
    key_down,
    key_up,
    value_down,
    value_up,
    out_proj,
):
    own_rows, heads, width = queries.shape
    tenants = prefix_lengths.shape[0]
    rank = key_down.shape[3]
    vdim = value_absorb.shape[2]
    lat = key_absorb.shape[2]
    span = latent_cache.shape[0]
    half = heads // 2
    rows = 2 * own_rows
    pairs = n_inner // 2
    index = lax.axis_index("inner")
    group = lax.axis_index("grp")
    core = index & 1
    pair = index >> 1

    def inner_swap(x, distance):
        return lax.ppermute(x, "inner", [(a, a ^ distance) for a in range(n_inner)])

    def grp_swap(x, distance):
        return lax.ppermute(x, "grp", [(a, a ^ distance) for a in range(n_grp)])

    far = list(range(pairs - 1, 0, -1))
    cache = latent_cache.T
    pair_queries = inner_swap(queries, 1)
    same_cache = [inner_swap(cache, 2 * distance) for distance in far]
    other_cache = [inner_swap(block, 1) for block in [cache] + same_cache]
    places = [0] + [2 * distance for distance in far]
    places = places + [1 ^ place for place in places]
    place = jnp.concatenate(
        [jnp.bitwise_xor(index.astype(jnp.int32), jnp.array(places, jnp.int32)), core[None].astype(jnp.int32)]
    )

    ids = lax.dynamic_slice_in_dim(tenant_ids, pair * rows, rows, 0)
    table = ids[:, None] == (jnp.arange(tenants * rank, dtype=jnp.int32) // rank)[None, :]
    chosen = table.astype(F32)
    limits = jnp.sum(
        jnp.where(ids[:, None] == jnp.arange(tenants, dtype=jnp.int32)[None, :], prefix_lengths[None, :], 0), axis=1
    )
    limits = jnp.broadcast_to(limits[:, None], (rows, span))

    absorbed = pl.pallas_call(
        absorb_kernel,
        out_shape=jax.ShapeDtypeStruct((half * rows, lat + ROPE), BF16),
        grid_spec=pltpu.PrefetchScalarGridSpec(
            num_scalar_prefetch=1,
            grid=(1,),
            in_specs=[
                pl.BlockSpec(queries.shape, lambda i, s: (0, 0, 0)),
                pl.BlockSpec(queries.shape, lambda i, s: (0, 0, 0)),
                pl.BlockSpec(chosen.shape, lambda i, s: (0, 0)),
                pl.BlockSpec((half, NOPE, lat), lambda i, s: (s[0], 0, 0)),
                pl.BlockSpec((tenants, half, rank, NOPE), lambda i, s: (0, s[0], 0, 0)),
                pl.BlockSpec((tenants, half, rank, lat), lambda i, s: (0, s[0], 0, 0)),
            ],
            out_specs=pl.BlockSpec((half * rows, lat + ROPE), lambda i, s: (0, 0)),
            scratch_shapes=[pltpu.VMEM((rows * heads, NOPE), F32)] * 2,
        ),
        compiler_params=pltpu.CompilerParams(vmem_limit_bytes=16 << 20),
        cost_estimate=cost(2 * half * rows * lat * (NOPE + 2 * tenants * rank), 4 << 20),
        name="absorb",
    )(core[None].astype(jnp.int32), queries, pair_queries, chosen, key_absorb, key_down.transpose(0, 1, 3, 2), key_up)

    blocks = [cache] + same_cache + other_cache
    head_out = pl.pallas_call(
        functools.partial(attend_kernel, len(blocks), width ** -0.5),
        out_shape=jax.ShapeDtypeStruct((rows, half * vdim), BF16),
        in_specs=[spec(SMEM)] + [spec(VMEM)] * (3 + len(blocks)) + [spec(HBM)] * 3,
        out_specs=spec(VMEM),
        scratch_shapes=[
            pltpu.VMEM((half * rows, len(blocks) * span), F32),
            pltpu.VMEM((half * rows, len(blocks) * span), BF16),
            pltpu.VMEM((half, lat, vdim), BF16),
            pltpu.VMEM((tenants, half, rank, lat), BF16),
            pltpu.VMEM((tenants, half, rank, vdim), BF16),
            pltpu.SemaphoreType.DMA((3,)),
        ],
        compiler_params=pltpu.CompilerParams(vmem_limit_bytes=32 << 20),
        cost_estimate=cost(4 * half * rows * lat * len(blocks) * span, 8 << 20),
        name="attend",
    )(place, absorbed, limits, chosen, *blocks, value_absorb, value_down.transpose(0, 1, 3, 2), value_up)

    same = [head_out] + [None] * (pairs - 1)
    other = [None] * pairs
    for distance in far:
        same[distance] = inner_swap(head_out, 2 * distance)
    for distance in range(pairs):
        other[distance] = inner_swap(same[distance], 1)
    where = jnp.stack([core, pair, group]).astype(jnp.int32)
    total = pairs * rows
    chunk = total // n_grp
    columns = out_proj.shape[1]
    keep, send = pl.pallas_call(
        functools.partial(project_kernel, pairs, n_grp),
        out_shape=(
            jax.ShapeDtypeStruct((chunk, columns), F32),
            jax.ShapeDtypeStruct((n_grp - 1, chunk, columns), BF16),
        ),
        in_specs=[spec(SMEM)] + [spec(VMEM)] * (2 * pairs + 1),
        out_specs=(spec(VMEM), spec(VMEM)),
        scratch_shapes=[pltpu.VMEM((total, 2 * half * vdim), BF16)],
        compiler_params=pltpu.CompilerParams(vmem_limit_bytes=16 << 20),
        cost_estimate=cost(2 * total * columns * 2 * half * vdim, 8 << 20),
        name="project",
    )(where, *same, *other, out_proj)
    result = keep
    for distance in range(n_grp - 1, 0, -1):
        result = result + grp_swap(send[distance - 1], distance).astype(F32)
    return result.astype(BF16)


def solution(mesh):
    in_specs = (
        P("inner", "grp", None),
        P(),
        P(),
        P("inner", None),
        P("grp", None, None),
        P("grp", None, None),
        P(None, "grp", None, None),
        P(None, "grp", None, None),
        P(None, "grp", None, None),
        P(None, "grp", None, None),
        P("grp", "inner"),
    )
    body = functools.partial(local, mesh.shape["inner"], mesh.shape["grp"])
    return jax.shard_map(body, mesh=mesh, in_specs=in_specs, out_specs=P("grp", "inner"), check_vma=False)
```
